16 devices in a mesh: dp: 2 (over y, z), tp: 8 (over x, core).
Axes of the slice: x: 4, y: 2, z: 1, core: 2. Of those that a mesh axis runs over, the one named last changes fastest.
The devices are a block of a 4x4x8 slice.
Arguments:
- x: bfloat16 [8192, 2048], P(('dp', 'tp')), parts along dimension 0
- dy: bfloat16 [8192, 2048], P(('dp', 'tp')), parts along dimension 0
- gain: bfloat16 [2048], replicated
- wq: bfloat16 [2048, 4096], P(None, 'tp')
- wk: bfloat16 [2048, 2048], P(None, 'tp')
- wv: bfloat16 [2048, 2048], P(None, 'tp')
- wo: bfloat16 [4096, 2048], P('tp')
Outputs:
- output 1: bfloat16 [8192, 2048], P(('dp', 'tp')), parts along dimension 0
- output 2: float32 [2, 2048], P('dp'), parts along dimension 0
- output 3: bfloat16 [4096, 4096], P('dp', 'tp'), parts along dimension 0
- output 4: bfloat16 [4096, 2048], P('dp', 'tp'), parts along dimension 0
- output 5: bfloat16 [4096, 2048], P('dp', 'tp'), parts along dimension 0
- output 6: bfloat16 [8192, 2048], P(('dp', 'tp')), parts along dimension 0
There are 2 independent parts. The reference program is written for one: setup_inputs(seed, part) draws one part's arguments, and reference() takes and returns one part's arrays. A program takes and returns all parts, laid end to end along the dimension named above; an argument that names none is the same for every part.
All inputs are finite; a program needn't handle non-finite values.
Results may differ from the reference program's by a relative error of at most 0.018.
Values are sent between devices in bfloat16 or wider.
A program may use at most 768 MiB of HBM per device.

```python
import jax
import jax.numpy as jnp
from jax import lax

ROWS = 4096
D = 2048
HEADS = 32
KV_HEADS = 16
HEAD = 128
THETA = 10000


def setup_inputs(seed: int = 0, part: int = 0) -> dict:
    kx, ky, kn, kq, kk, kv, ko = jax.random.split(jax.random.key(seed), 7)

    def weights(key, rows, columns):
        return jax.random.normal(key, (rows, columns), jnp.float32) * rows**-0.5

    drawn = {
        "x": jax.random.normal(jax.random.fold_in(kx, part), (ROWS, D), jnp.float32),
        "dy": jax.random.normal(jax.random.fold_in(ky, part), (ROWS, D), jnp.float32) * ROWS**-0.5,
        "gain": 1 + 0.1 * jax.random.normal(kn, (D,), jnp.float32),
        "wq": 2 * weights(kq, D, HEADS * HEAD),
        "wk": 2 * weights(kk, D, KV_HEADS * HEAD),
        "wv": 4 * weights(kv, D, KV_HEADS * HEAD),
        "wo": weights(ko, HEADS * HEAD, D),
    }
    return {k: v.astype(jnp.bfloat16) for k, v in drawn.items()}


def normed(x, gain):
    wide = x.astype(jnp.float32)
    scale = lax.rsqrt(jnp.mean(wide * wide, -1, keepdims=True) + 1e-6)
    return (wide * scale * gain.astype(jnp.float32)).astype(jnp.bfloat16)


def turned(t, place, theta):
    half = t.shape[-1] // 2
    angle = place.astype(jnp.float32)[:, None] * theta ** (-jnp.arange(half, dtype=jnp.float32) / half)
    cos, sin = jnp.cos(angle)[:, None], jnp.sin(angle)[:, None]
    a, b = t[..., :half].astype(jnp.float32), t[..., half:].astype(jnp.float32)
    return jnp.concatenate([a * cos - b * sin, b * cos + a * sin], -1).astype(jnp.bfloat16)


def matmul(a, w):
    return jnp.dot(a, w, preferred_element_type=jnp.float32).astype(jnp.bfloat16)


def einsum(form, a, b):
    return jnp.einsum(form, a.astype(jnp.float32), b.astype(jnp.float32))


def attention(q, k, v):
    scores = einsum("tgsd,ugd->gstu", q, k) * q.shape[-1] ** -0.5
    token = jnp.arange(q.shape[0])
    scores = jnp.where(token[:, None] >= token, scores, -jnp.inf)
    weights = jax.nn.softmax(scores, -1).astype(jnp.bfloat16)
    return einsum("gstu,ugd->tgsd", weights, v).astype(jnp.bfloat16)


def forward(x, gain, wq, wk, wv, wo):
    rows = x.shape[0]
    a, place = normed(x, gain), jnp.arange(rows)
    k = turned(matmul(a, wk).reshape(rows, -1, HEAD), place, THETA)
    q = turned(matmul(a, wq).reshape(rows, -1, HEAD), place, THETA).reshape(rows, k.shape[1], -1, HEAD)
    v = matmul(a, wv).reshape(rows, -1, HEAD)
    seen = attention(q, k, v).reshape(rows, -1)
    return (x.astype(jnp.float32) + jnp.dot(seen, wo, preferred_element_type=jnp.float32)).astype(jnp.bfloat16)


def reference(x, dy, gain, wq, wk, wv, wo):
    _, back = jax.vjp(forward, x, gain.astype(jnp.float32), wq, wk, wv, wo)
    by_x, by_gain, *by_weights = back(dy)
    return (by_x, by_gain[None], *by_weights)
```

```python
import functools

import jax
import jax.numpy as jnp
import numpy as np
from jax import lax
from jax.experimental import pallas as pl
from jax.experimental.pallas import tpu as pltpu

NEG = -1e30
HIDDEN = 2 * NEG
LOG2E = 1.4426950408889634


def _dot(a, b, ca, cb):
    return lax.dot_general(a, b, (((ca,), (cb,)), ((), ())), preferred_element_type=jnp.float32)


from jax.sharding import PartitionSpec as P

HEAD = 128
THETA = 10000
MESH = pl.DeviceIdType.MESH

OWN, L0, L1, R0, R1, O0, O1, LP, RP, OP = range(10)


def _place(n, me, size):
    flip = jnp.where((n == 1) | (n == 4) | (n == 5) | (n == 7), 1, 0)
    step = jnp.where(n < 2, 0, jnp.where(n >= 6, 4, jnp.where((n == 2) | (n == 4), size - 2, 2)))
    core = lax.rem(me, 2)
    return lax.rem(me - core + step, size) + lax.rem(core + flip, 2)


def _gather_forward(size, x_ref, gain_ref, rate_ref, dy_in, wq_in, wk_in, wv_in, wo_in,
                    xa_ref, dya_ref, q_out, k_out, v_out, do_out, lse_ref, delta_ref, dwo_ref, low_ref, high_ref,
                    dy_ref, wq_ref, wk_ref, wv_ref, wo_ref, q_ref, k_ref, v_ref, do_ref, xn_s, buf_s, vt_s, top_s, mix_s, o_s, dwo_s,
                    send_sem, recv_sem, load_sem, own_sem, fetch_sem, save_sem, do_sem):
    rows, d = x_ref.shape
    half = rows // 2
    kb, g = k_ref.shape[0], q_ref.shape[1] // k_ref.shape[1]
    cols = g * rows
    me = lax.axis_index("tp")
    core = lax.rem(me, 2)
    partner = me + 1 - 2 * core
    right, left = lax.rem(me + 2, size), lax.rem(me + size - 2, size)
    opposite = lax.rem(me + 4, size)
    e = HEAD**-0.5 * LOG2E
    all_refs, own_refs = (xa_ref, dya_ref), (xn_s, dy_ref)

    fetches = [pltpu.make_async_copy(a, b, fetch_sem.at[n]) for n, (a, b) in enumerate(
        ((dy_in, dy_ref), (wq_in, wq_ref), (wk_in, wk_ref), (wv_in, wv_ref), (wo_in, wo_ref)))]
    for fetch in fetches:
        fetch.start()
    barrier = pltpu.get_barrier_semaphore()
    for other in (partner, left, right):
        pl.semaphore_signal(barrier, inc=1, device_id={"tp": other}, device_id_type=MESH)

    def at(unit, part=0, count=rows):
        return pl.ds(pl.multiple_of(unit * rows + part * half, half), count)

    def copy(a, event, src, dst_rows, target):
        return pltpu.make_async_remote_copy(src_ref=src, dst_ref=all_refs[a].at[dst_rows], send_sem=send_sem.at[a, event],
                                            recv_sem=recv_sem.at[a, event], device_id={"tp": target}, device_id_type=MESH)

    def sent(a, event):
        own, land = own_refs[a], all_refs[a]
        if event == OWN:
            return copy(a, event, own, at(me), partner)
        if event in (L0, L1):
            h = event - L0
            return copy(a, event, own.at[pl.ds(h * half, half)], at(me, h, half), right)
        if event in (R0, R1):
            h = event - R0
            return copy(a, event, own.at[pl.ds(h * half, half)], at(me, h, half), left)
        if event == O0:
            return copy(a, event, land.at[at(left, 0, half)], at(left, 0, half), right)
        if event == O1:
            return copy(a, event, land.at[at(right, 1, half)], at(right, 1, half), left)
        unit = {LP: left, RP: right, OP: opposite}[event]
        return copy(a, event, land.at[at(unit)], at(unit), partner)

    def arrived(a, event):
        if event in (OWN, LP, RP, OP):
            base = me - core + (1 - core)
            unit = {OWN: base, LP: lax.rem(base + size - 2, size), RP: lax.rem(base + 2, size), OP: lax.rem(base + 4, size)}[event]
            where = at(unit)
        else:
            unit, h = {L0: (left, 0), L1: (left, 1), R0: (right, 0), R1: (right, 1), O0: (opposite, 0), O1: (opposite, 1)}[event]
            where = at(unit, h, half)
        copy(a, event, all_refs[a].at[where], where, partner).wait_recv()

    def load(a, n):
        return pltpu.make_async_copy(all_refs[a].at[at(_place(n, me, size))], buf_s.at[lax.rem(n, 2)], load_sem.at[lax.rem(n, 2)])

    def keep(a):
        return pltpu.make_async_copy(own_refs[a], all_refs[a].at[at(me)], own_sem.at[a])

    def norm(j, _):
        here = pl.ds(pl.multiple_of(j * 128, 128), 128)
        wide = x_ref[here, :].astype(jnp.float32)
        scale = lax.rsqrt(jnp.mean(wide * wide, -1, keepdims=True) + 1e-6)
        xn_s[here, :] = (wide * scale * gain_ref[...]).astype(jnp.bfloat16)

    lax.fori_loop(0, rows // 128, norm, None)
    pl.semaphore_wait(barrier, 3)
    for event in (L0, R1, L1, R0, OWN):
        sent(0, event).start()
    keep(0).start()

    for ref, apart in ((low_ref, 1), (high_ref, rows)):
        angle = (lax.broadcasted_iota(jnp.int32, ref.shape[1:], 0) * apart).astype(jnp.float32) * rate_ref[...]
        ref[0] = jnp.cos(angle)
        ref[1] = jnp.sin(angle)
    for fetch in fetches:
        fetch.wait()
    keep(1).start()
    sent(1, OWN).start()

    top_s[...] = jnp.full(top_s.shape, NEG, jnp.float32)
    vt_s[:, HEAD:, :] = jnp.ones((kb, vt_s.shape[1] - HEAD, vt_s.shape[2]), vt_s.dtype)

    def clear(j, _):
        for i in range(kb):
            mix_s[i, :, pl.ds(pl.multiple_of(j * 512, 512), 512)] = jnp.zeros((mix_s.shape[1], 512), jnp.float32)

    lax.fori_loop(0, mix_s.shape[2] // 512, clear, None)

    def project(n, unit):
        a = buf_s[lax.rem(n, 2)]
        hc, hs = high_ref[0, pl.ds(unit, 1), :], high_ref[1, pl.ds(unit, 1), :]
        cos = low_ref[0] * hc - low_ref[1] * hs
        sin = low_ref[1] * hc + low_ref[0] * hs
        sign = jnp.where(lax.broadcasted_iota(jnp.int32, (1, HEAD), 1) < HEAD // 2, -1.0, 1.0)
        sin = sin * sign

        def turn(t):
            t = t.astype(jnp.bfloat16).astype(jnp.float32)
            return (t * cos + pltpu.roll(t, HEAD // 2, 1) * sin).astype(jnp.bfloat16)

        q = _dot(a, wq_ref[...], 1, 0)
        for i in range(kb):
            for j in range(g):
                h = i * g + j
                q_ref[i, pl.ds(pl.multiple_of(unit * cols + j * rows, rows), rows), :] = turn(q[:, h * HEAD : (h + 1) * HEAD])
        k = _dot(a, wk_ref[...], 1, 0)
        v = _dot(a, wv_ref[...], 1, 0)
        for i in range(kb):
            k_ref[i, at(unit), :] = turn(k[:, i * HEAD : (i + 1) * HEAD])
            own = v[:, i * HEAD : (i + 1) * HEAD].astype(jnp.bfloat16)
            v_ref[i, at(unit), :] = own
            vt_s[i, :HEAD, at(unit)] = own.T

    def pair(pq, pk, masked):
        keys = at(pk)
        pieces = [(i, j) for i in range(kb) for j in range(g)]
        spots = [pl.ds(pl.multiple_of(pq * cols + j * rows, rows), rows) for _, j in pieces]
        scores = [_dot(k_ref[i, keys, :], q_ref[i, spot, :], 1, 1) for (i, _), spot in zip(pieces, spots)]
        if masked:
            ok = lax.broadcasted_iota(jnp.int32, (rows, rows), 1) >= lax.broadcasted_iota(jnp.int32, (rows, rows), 0)
        weights, keeps = [], []
        for (i, _), spot, s in zip(pieces, spots, scores):
            if masked:
                s = jnp.where(ok, s, HIDDEN)
            old = top_s[i : i + 1, spot]
            top = jnp.maximum(old, s.max(axis=0, keepdims=True))
            top_s[i : i + 1, spot] = top
            weights.append(jnp.exp2((s - top) * e).astype(jnp.bfloat16))
            keeps.append(jnp.exp2((old - top) * e))
        for (i, _), spot, p, was in zip(pieces, spots, weights, keeps):
            mix_s[i, :, spot] = mix_s[i, :, spot] * was + _dot(vt_s[i, :, keys], p, 1, 0)

    def passed_on(a):
        arrived(a, L0)
        sent(a, O0).start()
        arrived(a, R1)
        sent(a, O1).start()

    def sides(a):
        arrived(a, L1)
        sent(a, LP).start()
        arrived(a, R0)
        sent(a, RP).start()

    def far(a):
        arrived(a, O0)
        arrived(a, O1)
        sent(a, OP).start()

    keep(0).wait()
    load(0, 0).start()

    def unit_step(n, _):
        unit = _place(n, me, size)
        load(0, n).wait()
        for event, when in ((None, 2), (LP, 3), (RP, 4)):
            @pl.when(n == when)
            def _():
                if event is not None:
                    arrived(0, event)
                load(0, n + 1).start()

        project(n, unit)

        def earlier(m, _):
            other = _place(m, me, size)
            pair(jnp.maximum(unit, other), jnp.minimum(unit, other), False)

        lax.fori_loop(0, n, earlier, None)
        pair(unit, unit, True)

        @pl.when(n == 0)
        def _():
            arrived(0, OWN)
            load(0, n + 1).start()

        @pl.when(n == 1)
        def _():
            passed_on(0)
            sides(0)
            for event in (L0, R1, L1, R0):
                sent(1, event).start()
            load(0, n + 1).start()

        @pl.when(n == 5)
        def _():
            far(0)
            load(0, n + 1).start()

        @pl.when(n == 6)
        def _():
            passed_on(1)
            arrived(0, OP)
            load(0, n + 1).start()

    lax.fori_loop(0, size, unit_step, None)
    saves = [pltpu.make_async_copy(a, b, save_sem.at[n]) for n, (a, b) in enumerate(((q_ref, q_out), (k_ref, k_out), (v_ref, v_out)))]
    for save in saves:
        save.start()
    keep(1).wait()
    load(1, 0).start()

    def save_do(n):
        here = pl.ds(pl.multiple_of(_place(n, me, size) * cols, cols), cols)
        return pltpu.make_async_copy(do_ref.at[:, here], do_out.at[:, here], do_sem.at[n])

    def finish(unit, _):
        for i in range(kb):
            for j in range(g):
                spot = pl.ds(pl.multiple_of(unit * cols + j * rows, rows), rows)
                total = mix_s[i, HEAD : HEAD + 1, spot]
                o = (mix_s[i, :HEAD, spot] * (1 / total)).T.astype(jnp.bfloat16)
                h = i * g + j
                o_s[at(unit), h * HEAD : (h + 1) * HEAD] = o
                lse_ref[i : i + 1, spot] = top_s[i : i + 1, spot] * HEAD**-0.5 + jnp.log(total)

    lax.fori_loop(0, size, finish, None)
    dwo_s[...] = jnp.zeros_like(dwo_s)

    def dy_step(n, _):
        unit = _place(n, me, size)
        load(1, n).wait()
        for event, when in ((None, 2), (LP, 3), (RP, 4)):
            @pl.when(n == when)
            def _():
                if event is not None:
                    arrived(1, event)
                load(1, n + 1).start()

        slot = lax.rem(n, 2)
        by_o = _dot(buf_s[slot], wo_ref[...], 1, 1).astype(jnp.bfloat16)
        o = o_s[at(unit), :]
        for i in range(kb):
            for j in range(g):
                h = i * g + j
                spot = pl.ds(pl.multiple_of(unit * cols + j * rows, rows), rows)
                mine = by_o[:, h * HEAD : (h + 1) * HEAD]
                do_ref[i, spot, :] = mine
                prod = mine.astype(jnp.float32) * o[:, h * HEAD : (h + 1) * HEAD].astype(jnp.float32)
                delta_ref[i : i + 1, spot] = prod.T.sum(axis=0, keepdims=True)

        save_do(n).start()

        def some(c, _):
            here = pl.ds(pl.multiple_of(c * 512, 512), 512)
            dwo_s[:, here] += _dot(o, buf_s[slot, :, here], 0, 0)

        lax.fori_loop(0, d // 512, some, None)

        @pl.when(n == 0)
        def _():
            arrived(1, OWN)
            load(1, n + 1).start()

        @pl.when(n == 1)
        def _():
            sides(1)
            load(1, n + 1).start()

        @pl.when(n == 5)
        def _():
            far(1)
            load(1, n + 1).start()

        @pl.when(n == 6)
        def _():
            arrived(1, OP)
            load(1, n + 1).start()

    lax.fori_loop(0, size, dy_step, None)
    dwo_ref[...] = dwo_s[...].astype(dwo_ref.dtype)
    for save in saves:
        save.wait()
    lax.fori_loop(0, size, lambda n, _: save_do(n).wait(), None)
    for a in range(2):
        for event in range(10):
            sent(a, event).wait_send()


def gather_forward(size, x, dy, gain, wq, wk, wv, wo):
    rows, d = x.shape
    total = rows * size
    kb, heads = wk.shape[1] // HEAD, wq.shape[1] // HEAD
    half = HEAD // 2
    rate = np.tile(np.float32(THETA) ** (-np.arange(half, dtype=np.float32) / half), 2)[None]
    bf16, f32 = jnp.bfloat16, jnp.float32
    vmem, hbm = pl.BlockSpec(memory_space=pltpu.VMEM), pl.BlockSpec(memory_space=pl.ANY)
    shape, dma = jax.ShapeDtypeStruct, pltpu.SemaphoreType.DMA
    width = heads // kb * total
    by_q, by_k, stats = (kb, width, HEAD), (kb, total, HEAD), (kb, width)
    return pl.pallas_call(
        functools.partial(_gather_forward, size),
        in_specs=[vmem] * 3 + [hbm] * 5,
        out_specs=[hbm] * 6 + [vmem] * 5,
        out_shape=[shape(s, bf16) for s in ((total, d), (total, d), by_q, by_k, by_k, by_q)]
        + [shape(stats, f32), shape(stats, f32), shape(wo.shape, bf16), shape((2, rows, HEAD), f32), shape((2, size, HEAD), f32)],
        scratch_shapes=[pltpu.VMEM(s, bf16) for s in (x.shape, wq.shape, wk.shape, wv.shape, wo.shape, by_q, by_k, by_k, by_q, x.shape,
                                                      (2, rows, d), (kb, HEAD + 16, total))]
        + [pltpu.VMEM(stats, f32), pltpu.VMEM((kb, HEAD + 16, width), f32), pltpu.VMEM((total, heads * HEAD), bf16), pltpu.VMEM(wo.shape, f32)]
        + [dma(s) for s in ((2, 10), (2, 10), (2,), (2,), (5,), (3,), (size,))],
        compiler_params=pltpu.CompilerParams(collective_id=0, has_side_effects=True, vmem_limit_bytes=62 * 2**20),
    )(x, gain.astype(f32)[None], jnp.asarray(rate), dy, wq, wk, wv, wo)


POINTS = (("", "", "70", "", "6071", "", "507261", "", "40736251", "", "30", "", "20635241", "", "1031", "", "00", "", "534221", "", "", "3211", "", "014322331202231303"),
          ("", "", "70", "", "6071", "", "507261", "", "40736251", "", "30", "", "20635241", "", "1031", "", "00", "", "534221", "", "", "3211", "", "014322331202231303"))
ORDER = [[(int(a), int(b)) for point in points for a, b in zip(point[::2], point[1::2])] for points in POINTS]
STARTS = [[sum(len(point) for point in points[:n]) // 2 for n in range(len(points) + 1)] for points in POINTS]


def _pick(index, values):
    got = values[0]
    for n in range(1, len(values)):
        got = jnp.where(index == n, values[n], got)
    return got


def _backward(size, gain_ref, lse_ref, delta_ref, low_ref, high_ref, wq_in, wk_in, wv_in, q_ref, k_ref, v_ref, do_ref, xa_ref, x_ref, dy_ref,
              dx_ref, dgain_ref, dwq_ref, dwk_ref, dwv_ref,
              wq_ref, wk_ref, wv_ref, q_s, k_s, v_s, do_s, dq_s, dk_s, dv_s, tile_s, term_s, out_s, in_s, chain_s, last_s, stage_s, gain_s, gains_s,
              load_sem, do_sem, tile_sem, stage_sem, x_sem, out_sem, in_sem, chain_send, chain_recv, last_recv, gain_send, gain_recv):
    rows, d = x_ref.shape
    part = d // 2
    kb, g = k_ref.shape[0], q_ref.shape[1] // k_ref.shape[1]
    cols = g * rows
    pieces = [(i, j) for i in range(kb) for j in range(g)]
    chips = size // 2
    me = lax.axis_index("tp")
    core = lax.rem(me, 2)
    chip = lax.div(me, 2)
    partner = me + 1 - 2 * core
    onward = lax.rem(me + jnp.where(core == 0, 2, size - 2), size)
    scale = HEAD**-0.5
    e = scale * LOG2E
    bf16, f32 = jnp.bfloat16, jnp.float32
    subs = chain_recv.shape[1]
    sub = rows // subs

    barrier = pltpu.get_barrier_semaphore()
    for other in range(1, size):
        pl.semaphore_signal(barrier, inc=1, device_id={"tp": lax.rem(me + other, size)}, device_id_type=MESH)

    loads = [pltpu.make_async_copy(a, b, load_sem.at[n]) for n, (a, b) in enumerate(
        ((q_ref, q_s), (k_ref, k_s), (v_ref, v_s), (wq_in, wq_ref), (wk_in, wk_ref), (wv_in, wv_ref)))]
    for load in loads:
        load.start()

    def at(unit):
        return pl.ds(pl.multiple_of(unit * rows, rows), rows)

    def spot(unit, j):
        return pl.ds(pl.multiple_of(unit * cols + j * rows, rows), rows)

    def load_do(n):
        unit = size - 1 - n
        return pltpu.make_async_copy(do_ref.at[:, pl.ds(pl.multiple_of(unit * cols, cols), cols)], do_s.at[lax.rem(n, 2)], do_sem.at[lax.rem(n, 2)])

    def load_tile(n):
        width = tile_s.shape[2]
        return pltpu.make_async_copy(xa_ref.at[:, pl.ds(pl.multiple_of(n * width, width), width)], tile_s.at[lax.rem(n, 2)], tile_sem.at[lax.rem(n, 2)])

    load_do(0).start()

    def clear(j, _):
        for i in range(kb):
            dk_s[i, at(j), :] = jnp.zeros((rows, HEAD), f32)
            dv_s[i, at(j), :] = jnp.zeros((rows, HEAD), f32)

    lax.fori_loop(0, size, clear, None)
    pl.semaphore_wait(barrier, size - 1)
    for load in loads[:3]:
        load.wait()

    def pair(n, pq, pk, masked):
        slot = lax.rem(n, 2)
        keys = at(pk)
        if masked:
            ok = lax.broadcasted_iota(jnp.int32, (rows, rows), 1) >= lax.broadcasted_iota(jnp.int32, (rows, rows), 0)
        for i in range(kb):
            here = [slice(j * rows, (j + 1) * rows) for j in range(g)]
            qs = [q_s[i, spot(pq, j), :] for j in range(g)]
            dos = [do_s[slot, i, at_j, :] for at_j in here]
            scores = [_dot(k_s[i, keys, :], q, 1, 1) for q in qs]
            dps = [_dot(v_s[i, keys, :], do, 1, 1) for do in dos]
            for j in range(g):
                p = jnp.exp2(scores[j] * e - lse_ref[i : i + 1, spot(pq, j)] * LOG2E)
                if masked:
                    p = jnp.where(ok, p, 0.0)
                ds = (p * (dps[j] - delta_ref[i : i + 1, spot(pq, j)])).astype(bf16)
                dv_s[i, keys, :] += _dot(p.astype(bf16), dos[j], 1, 0)
                dk_s[i, keys, :] += _dot(ds, qs[j], 1, 0)
                new = _dot(k_s[i, keys, :].T, ds, 1, 0)
                dq_s[i, :, here[j]] = new if masked else dq_s[i, :, here[j]] + new

    def swap(unit):
        return pltpu.make_async_remote_copy(src_ref=out_s, dst_ref=in_s.at[unit], send_sem=out_sem, recv_sem=in_sem.at[unit],
                                            device_id={"tp": partner}, device_id_type=MESH)

    def pass_on(unit, s):
        here = pl.ds(s * sub, sub)
        return pltpu.make_async_remote_copy(src_ref=chain_s.at[unit, here], dst_ref=chain_s.at[unit, here], send_sem=chain_send.at[unit, s],
                                            recv_sem=chain_recv.at[unit, s], device_id={"tp": onward}, device_id_type=MESH)

    def hand_over(unit, s):
        here = pl.ds(s * sub, sub)
        return pltpu.make_async_remote_copy(src_ref=chain_s.at[unit, here], dst_ref=last_s.at[here], send_sem=chain_send.at[unit, s],
                                            recv_sem=last_recv.at[s], device_id={"tp": partner}, device_id_type=MESH)

    def turn_of(unit):
        away = jnp.where(core == 0, chip - lax.div(unit, 2), lax.div(unit, 2) - chip)
        return lax.rem(away + 2 * chips - 1, chips)

    def term(dq, dk, dv, first):
        here = pl.ds(pl.multiple_of(first, 256), 256)
        return _dot(dq, wq_ref[here, :], 1, 1) + _dot(dk, wk_ref[here, :], 1, 1) + _dot(dv, wv_ref[here, :], 1, 1)

    def by_heads(unit):
        dq = jnp.concatenate([q_s[i, spot(unit, j), :] for i, j in pieces], axis=1)
        return dq, *(jnp.concatenate([ref[i, at(unit), :] for i in range(kb)], axis=1) for ref in (k_s, v_s))

    def add_up(index, _):
        unit, turn = (jnp.where(core == 0, *(_pick(index, [entry[m] for entry in order]) for order in ORDER)) for m in range(2))

        @pl.when(turn_of(unit) == turn)
        def _():
            grads = by_heads(unit)
            for c in range(0, part, 256):
                term_s[:, c : c + 256] = term(*grads, core * part + c)
            swap(unit).wait_recv()
            for s in range(subs):
                here = pl.ds(s * sub, sub)
                mine = term_s[here, :] + in_s[unit, here, :].astype(f32)

                @pl.when(turn == 0)
                def _():
                    chain_s[unit, here, :] = mine.astype(bf16)

                @pl.when(turn > 0)
                def _():
                    pass_on(unit, s).wait_recv()
                    chain_s[unit, here, :] = (mine + chain_s[unit, here, :].astype(f32)).astype(bf16)

                @pl.when(turn < chips - 1)
                def _():
                    pass_on(unit, s).start()

                @pl.when((turn == chips - 1) & (lax.rem(unit, 2) != core))
                def _():
                    hand_over(unit, s).start()

    def point(n):
        first, end = (jnp.where(core == 0, *(_pick(at_n, starts) for starts in STARTS)) for at_n in (n, n + 1))
        lax.fori_loop(first, end, add_up, None)

    def step(n, _):
        unit = size - 1 - n
        load_do(n).wait()

        @pl.when(n < size - 1)
        def _():
            load_do(n + 1).start()

        pair(n, unit, unit, True)
        point(2 * n)
        lax.fori_loop(0, unit, lambda m, _: pair(n, unit, m, False), None)
        point(2 * n + 1)

        hc, hs = high_ref[0, pl.ds(unit, 1), :], high_ref[1, pl.ds(unit, 1), :]
        cos = low_ref[0] * hc - low_ref[1] * hs
        sin = low_ref[1] * hc + low_ref[0] * hs
        sin = sin * jnp.where(lax.broadcasted_iota(jnp.int32, (1, HEAD), 1) < HEAD // 2, 1.0, -1.0)

        def turn_back(t):
            t = (t * scale).astype(bf16).astype(f32)
            return (t * cos + pltpu.roll(t, HEAD // 2, 1) * sin).astype(bf16)

        for i, j in pieces:
            q_s[i, spot(unit, j), :] = turn_back(dq_s[i, :, j * rows : (j + 1) * rows].T)
        for i in range(kb):
            k_s[i, at(unit), :] = turn_back(dk_s[i, at(unit), :])
            v_s[i, at(unit), :] = dv_s[i, at(unit), :].astype(bf16)
        grads = by_heads(unit)

        @pl.when(n == 0)
        def _():
            for load in loads[3:]:
                load.wait()

        @pl.when(n > 0)
        def _():
            swap(unit).wait_send()

        for c in range(0, part, 256):
            out_s[:, c : c + 256] = term(*grads, (1 - core) * part + c).astype(bf16)
        swap(unit).start()

    lax.fori_loop(0, size, step, None)
    load_tile(0).start()
    swap(0).wait_send()
    width = tile_s.shape[2]
    tiles = d // width

    def late(m):
        return [pltpu.make_async_copy((x_ref, dy_ref)[m].at[:, pl.ds(n * width, width)], tile_s.at[m, pl.ds(n * rows, rows)], x_sem.at[m, n])
                for n in range(tiles)]


    def saves(n):
        slot, here, first = lax.rem(n, 2), pl.ds(pl.multiple_of(n * tile_s.shape[2], tile_s.shape[2]), tile_s.shape[2]), 0
        copies = []
        for m, ref in enumerate((dwq_ref, dwk_ref, dwv_ref)):
            copies.append(pltpu.make_async_copy(stage_s.at[slot, :, pl.ds(first, ref.shape[1])], ref.at[here, :], stage_sem.at[slot, m]))
            first += ref.shape[1]
        return copies

    def weights(n, _):
        width = tile_s.shape[2]
        load_tile(n).wait()

        @pl.when(n < tiles - 1)
        def _():
            load_tile(n + 1).start()

        here = pl.ds(pl.multiple_of(n * width, width), width)
        a = tile_s[lax.rem(n, 2)]
        slot = lax.rem(n, 2)

        @pl.when(n > 1)
        def _():
            for save in saves(n - 2):
                save.wait()

        for i in range(kb):
            total = 0
            for unit in range(size):
                b = jnp.concatenate([q_s[i, unit * cols + j * rows : unit * cols + (j + 1) * rows, :] for j in range(g)], axis=1)
                total += _dot(a[unit * rows : (unit + 1) * rows], b, 0, 0)
            stage_s[slot, :, i * g * HEAD : (i + 1) * g * HEAD] = total.astype(bf16)
        for m, ref in enumerate((k_s, v_s)):
            b = jnp.concatenate([ref[i] for i in range(kb)], axis=1)
            first = kb * g * HEAD + m * kb * HEAD
            stage_s[slot, :, first : first + kb * HEAD] = _dot(a, b, 0, 0).astype(bf16)
        for save in saves(n):
            save.start()
        for m in range(2):
            @pl.when(n == tiles - 2 + m)
            def _():
                for load in late(m):
                    load.start()

        point(2 * size + n)

    lax.fori_loop(0, tiles, weights, None)

    for s in range(subs):
        hand_over(me, s).wait_recv()

    gain_s[...] = jnp.zeros_like(gain_s)
    for load in late(0) + late(1):
        load.wait()

    def norm(j, _):
        here = pl.ds(pl.multiple_of(j * 64, 64), 64)
        mine, other = chain_s[me, here, :], last_s[here, :]
        by = jnp.concatenate([jnp.where(core == 0, mine, other), jnp.where(core == 0, other, mine)], axis=1).astype(f32)
        wide, given = (jnp.concatenate([tile_s[m, pl.ds(n * rows + j * 64, 64)] for n in range(tiles)], axis=1).astype(f32) for m in range(2))
        size_of = lax.rsqrt(jnp.mean(wide * wide, -1, keepdims=True) + 1e-6)
        normal = wide * size_of
        gain_s[...] += (by * normal).reshape(8, 8, d).sum(axis=0)
        by = by * gain_ref[...]
        by = size_of * (by - normal * jnp.mean(by * normal, -1, keepdims=True))
        by = (by + given).astype(bf16)
        in_s[0, here, :], in_s[1, here, :] = by[:, :part], by[:, part:]

    lax.fori_loop(0, rows // 64, norm, None)

    def tell(other):
        return pltpu.make_async_remote_copy(src_ref=gain_s, dst_ref=gains_s.at[me], send_sem=gain_send.at[other], recv_sem=gain_recv.at[other],
                                            device_id={"tp": lax.rem(me + other, size)}, device_id_type=MESH)

    def heard(other):
        source = lax.rem(me + size - other, size)
        return pltpu.make_async_remote_copy(src_ref=gain_s, dst_ref=gains_s.at[source], send_sem=gain_send.at[other], recv_sem=gain_recv.at[other],
                                            device_id={"tp": lax.rem(me + other, size)}, device_id_type=MESH)

    for other in range(1, size):
        tell(other).start()
    results = [pltpu.make_async_copy(in_s.at[n], dx_ref.at[:, pl.ds(n * part, part)], x_sem.at[0, n]) for n in range(2)]
    for save in results:
        save.start()
    gains_s[me] = gain_s[...]
    for other in range(1, size):
        heard(other).wait_recv()
    total = gains_s[0]
    for other in range(1, size):
        total += gains_s[other]
    dgain_ref[...] = total.sum(axis=0, keepdims=True)
    for other in range(1, size):
        tell(other).wait_send()
    for save in (*results, *saves(tiles - 2), *saves(tiles - 1)):
        save.wait()

    def sent(unit, _):
        final = turn_of(unit) == chips - 1

        @pl.when(jnp.logical_not(final))
        def _():
            for s in range(subs):
                pass_on(unit, s).wait_send()

        @pl.when(final & (lax.rem(unit, 2) != core))
        def _():
            for s in range(subs):
                hand_over(unit, s).wait_send()

    lax.fori_loop(0, size, sent, None)


def backward(size, x, dy, gain, lse, delta, wq, wk, wv, tables, q, k, v, do, xa):
    rows, d = x.shape
    kb, total = k.shape[:2]
    cols = q.shape[1] // size
    bf16, f32 = jnp.bfloat16, jnp.float32
    vmem, hbm = pl.BlockSpec(memory_space=pltpu.VMEM), pl.BlockSpec(memory_space=pl.ANY)
    shape, dma, subs, width = jax.ShapeDtypeStruct, pltpu.SemaphoreType.DMA, 4, 256
    return pl.pallas_call(
        functools.partial(_backward, size),
        in_specs=[vmem] * 5 + [hbm] * 10,
        out_specs=[hbm, vmem, hbm, hbm, hbm],
        out_shape=[shape((rows, d), bf16), shape((1, d), f32)] + [shape(w.shape, bf16) for w in (wq, wk, wv)],
        scratch_shapes=[pltpu.VMEM(w.shape, bf16) for w in (wq, wk, wv)] + [
                        pltpu.VMEM(q.shape, bf16), pltpu.VMEM(k.shape, bf16), pltpu.VMEM(v.shape, bf16), pltpu.VMEM((2, kb, cols, HEAD), bf16),
                        pltpu.VMEM((kb, HEAD, cols), f32), pltpu.VMEM(k.shape, f32), pltpu.VMEM(v.shape, f32), pltpu.VMEM((2, total, width), bf16),
                        pltpu.VMEM((rows, d // 2), f32), pltpu.VMEM((rows, d // 2), bf16), pltpu.VMEM((size, rows, d // 2), bf16),
                        pltpu.VMEM((size, rows, d // 2), bf16), pltpu.VMEM((rows, d // 2), bf16), pltpu.VMEM((2, width, sum(w.shape[1] for w in (wq, wk, wv))), bf16), pltpu.VMEM((8, d), f32),
                        pltpu.VMEM((size, 8, d), f32),
                        dma((6,)), dma((2,)), dma((2,)), dma((2, 3)), dma((2, d // width)), dma, dma((size,)), dma((size, subs)), dma((size, subs)), dma((subs,)), dma((size,)), dma((size,))],
        compiler_params=pltpu.CompilerParams(collective_id=1, has_side_effects=True, vmem_limit_bytes=67043328),
    )(gain.astype(f32)[None], lse, delta, *tables, wq, wk, wv, q, k, v, do, xa, x, dy)


def solution(mesh):
    size = mesh.shape["tp"]

    def step(x, dy, gain, wq, wk, wv, wo):
        xa, _, q, k, v, do, lse, delta, dwo, *tables = gather_forward(size, x, dy, gain, wq, wk, wv, wo)
        dx, dgain, dwq, dwk, dwv = backward(size, x, dy, gain, lse, delta, wq, wk, wv, tables, q, k, v, do, xa)
        return dx, dgain, dwq, dwk, dwv, dwo

    tokens, columns = P(("dp", "tp"), None), P(None, "tp")
    return jax.shard_map(
        step,
        mesh=mesh,
        in_specs=(tokens, tokens, P(None), columns, columns, columns, P("tp", None)),
        out_specs=(tokens, P("dp", None), P("dp", "tp"), P("dp", "tp"), P("dp", "tp"), P(("dp", "tp"), None)),
        check_vma=False,
    )
```

```python
import functools

import jax
import jax.numpy as jnp
import numpy as np
from jax import lax
from jax.experimental import pallas as pl
from jax.experimental.pallas import tpu as pltpu

NEG = -1e30
HIDDEN = 2 * NEG
LOG2E = 1.4426950408889634


def _dot(a, b, ca, cb):
    return lax.dot_general(a, b, (((ca,), (cb,)), ((), ())), preferred_element_type=jnp.float32)


from jax.sharding import PartitionSpec as P

HEAD = 128
THETA = 10000
MESH = pl.DeviceIdType.MESH

OWN, L0, L1, R0, R1, O0, O1, LP, RP, OP = range(10)


def _place(n, me, size):
    flip = jnp.where((n == 1) | (n == 4) | (n == 5) | (n == 7), 1, 0)
    step = jnp.where(n < 2, 0, jnp.where(n >= 6, 4, jnp.where((n == 2) | (n == 4), size - 2, 2)))
    core = lax.rem(me, 2)
    return lax.rem(me - core + step, size) + lax.rem(core + flip, 2)


def _gather_forward(size, x_ref, gain_ref, rate_ref, dy_in, wq_in, wk_in, wv_in, wo_in,
                    xa_ref, dya_ref, q_out, k_out, v_out, do_out, lse_ref, delta_ref, dwo_ref, low_ref, high_ref,
                    dy_ref, wq_ref, wk_ref, wv_ref, wo_ref, q_ref, k_ref, v_ref, do_ref, xn_s, buf_s, vt_s, top_s, mix_s, o_s, dwo_s,
                    send_sem, recv_sem, load_sem, own_sem, fetch_sem, save_sem, do_sem):
    rows, d = x_ref.shape
    half = rows // 2
    kb, g = k_ref.shape[0], q_ref.shape[1] // k_ref.shape[1]
    cols = g * rows
    me = lax.axis_index("tp")
    core = lax.rem(me, 2)
    partner = me + 1 - 2 * core
    right, left = lax.rem(me + 2, size), lax.rem(me + size - 2, size)
    opposite = lax.rem(me + 4, size)
    e = HEAD**-0.5 * LOG2E
    all_refs, own_refs = (xa_ref, dya_ref), (xn_s, dy_ref)

    fetches = [pltpu.make_async_copy(a, b, fetch_sem.at[n]) for n, (a, b) in enumerate(
        ((dy_in, dy_ref), (wq_in, wq_ref), (wk_in, wk_ref), (wv_in, wv_ref), (wo_in, wo_ref)))]
    for fetch in fetches:
        fetch.start()
    barrier = pltpu.get_barrier_semaphore()
    for other in (partner, left, right):
        pl.semaphore_signal(barrier, inc=1, device_id={"tp": other}, device_id_type=MESH)

    def at(unit, part=0, count=rows):
        return pl.ds(pl.multiple_of(unit * rows + part * half, half), count)

    def copy(a, event, src, dst_rows, target):
        return pltpu.make_async_remote_copy(src_ref=src, dst_ref=all_refs[a].at[dst_rows], send_sem=send_sem.at[a, event],
                                            recv_sem=recv_sem.at[a, event], device_id={"tp": target}, device_id_type=MESH)

    def sent(a, event):
        own, land = own_refs[a], all_refs[a]
        if event == OWN:
            return copy(a, event, own, at(me), partner)
        if event in (L0, L1):
            h = event - L0
            return copy(a, event, own.at[pl.ds(h * half, half)], at(me, h, half), right)
        if event in (R0, R1):
            h = event - R0
            return copy(a, event, own.at[pl.ds(h * half, half)], at(me, h, half), left)
        if event == O0:
            return copy(a, event, land.at[at(left, 0, half)], at(left, 0, half), right)
        if event == O1:
            return copy(a, event, land.at[at(right, 1, half)], at(right, 1, half), left)
        unit = {LP: left, RP: right, OP: opposite}[event]
        return copy(a, event, land.at[at(unit)], at(unit), partner)

    def arrived(a, event):
        if event in (OWN, LP, RP, OP):
            base = me - core + (1 - core)
            unit = {OWN: base, LP: lax.rem(base + size - 2, size), RP: lax.rem(base + 2, size), OP: lax.rem(base + 4, size)}[event]
            where = at(unit)
        else:
            unit, h = {L0: (left, 0), L1: (left, 1), R0: (right, 0), R1: (right, 1), O0: (opposite, 0), O1: (opposite, 1)}[event]
            where = at(unit, h, half)
        copy(a, event, all_refs[a].at[where], where, partner).wait_recv()

    def load(a, n):
        return pltpu.make_async_copy(all_refs[a].at[at(_place(n, me, size))], buf_s.at[lax.rem(n, 2)], load_sem.at[lax.rem(n, 2)])

    def keep(a):
        return pltpu.make_async_copy(own_refs[a], all_refs[a].at[at(me)], own_sem.at[a])

    def norm(j, _):
        here = pl.ds(pl.multiple_of(j * 128, 128), 128)
        wide = x_ref[here, :].astype(jnp.float32)
        scale = lax.rsqrt(jnp.mean(wide * wide, -1, keepdims=True) + 1e-6)
        xn_s[here, :] = (wide * scale * gain_ref[...]).astype(jnp.bfloat16)

    lax.fori_loop(0, rows // 128, norm, None)
    pl.semaphore_wait(barrier, 3)
    for event in (L0, R1, L1, R0, OWN):
        sent(0, event).start()
    keep(0).start()

    for ref, apart in ((low_ref, 1), (high_ref, rows)):
        angle = (lax.broadcasted_iota(jnp.int32, ref.shape[1:], 0) * apart).astype(jnp.float32) * rate_ref[...]
        ref[0] = jnp.cos(angle)
        ref[1] = jnp.sin(angle)
    for fetch in fetches:
        fetch.wait()
    keep(1).start()
    sent(1, OWN).start()

    top_s[...] = jnp.full(top_s.shape, NEG, jnp.float32)
    vt_s[:, HEAD:, :] = jnp.ones((kb, vt_s.shape[1] - HEAD, vt_s.shape[2]), vt_s.dtype)

    def clear(j, _):
        for i in range(kb):
            mix_s[i, :, pl.ds(pl.multiple_of(j * 512, 512), 512)] = jnp.zeros((mix_s.shape[1], 512), jnp.float32)

    lax.fori_loop(0, mix_s.shape[2] // 512, clear, None)

    def project(n, unit):
        a = buf_s[lax.rem(n, 2)]
        hc, hs = high_ref[0, pl.ds(unit, 1), :], high_ref[1, pl.ds(unit, 1), :]
        cos = low_ref[0] * hc - low_ref[1] * hs
        sin = low_ref[1] * hc + low_ref[0] * hs
        sign = jnp.where(lax.broadcasted_iota(jnp.int32, (1, HEAD), 1) < HEAD // 2, -1.0, 1.0)
        sin = sin * sign

        def turn(t):
            t = t.astype(jnp.bfloat16).astype(jnp.float32)
            return (t * cos + pltpu.roll(t, HEAD // 2, 1) * sin).astype(jnp.bfloat16)

        q = _dot(a, wq_ref[...], 1, 0)
        for i in range(kb):
            for j in range(g):
                h = i * g + j
                q_ref[i, pl.ds(pl.multiple_of(unit * cols + j * rows, rows), rows), :] = turn(q[:, h * HEAD : (h + 1) * HEAD])
        k = _dot(a, wk_ref[...], 1, 0)
        v = _dot(a, wv_ref[...], 1, 0)
        for i in range(kb):
            k_ref[i, at(unit), :] = turn(k[:, i * HEAD : (i + 1) * HEAD])
            own = v[:, i * HEAD : (i + 1) * HEAD].astype(jnp.bfloat16)
            v_ref[i, at(unit), :] = own
            vt_s[i, :HEAD, at(unit)] = own.T

    def pair(pq, pk, masked):
        keys = at(pk)
        pieces = [(i, j) for i in range(kb) for j in range(g)]
        spots = [pl.ds(pl.multiple_of(pq * cols + j * rows, rows), rows) for _, j in pieces]
        scores = [_dot(k_ref[i, keys, :], q_ref[i, spot, :], 1, 1) for (i, _), spot in zip(pieces, spots)]
        if masked:
            ok = lax.broadcasted_iota(jnp.int32, (rows, rows), 1) >= lax.broadcasted_iota(jnp.int32, (rows, rows), 0)
        weights, keeps = [], []
        for (i, _), spot, s in zip(pieces, spots, scores):
            if masked:
                s = jnp.where(ok, s, HIDDEN)
            old = top_s[i : i + 1, spot]
            top = jnp.maximum(old, s.max(axis=0, keepdims=True))
            top_s[i : i + 1, spot] = top
            weights.append(jnp.exp2((s - top) * e).astype(jnp.bfloat16))
            keeps.append(jnp.exp2((old - top) * e))
        for (i, _), spot, p, was in zip(pieces, spots, weights, keeps):
            mix_s[i, :, spot] = mix_s[i, :, spot] * was + _dot(vt_s[i, :, keys], p, 1, 0)

    def passed_on(a):
        arrived(a, L0)
        sent(a, O0).start()
        arrived(a, R1)
        sent(a, O1).start()

    def sides(a):
        arrived(a, L1)
        sent(a, LP).start()
        arrived(a, R0)
        sent(a, RP).start()

    def far(a):
        arrived(a, O0)
        arrived(a, O1)
        sent(a, OP).start()

    keep(0).wait()
    load(0, 0).start()

    def unit_step(n, _):
        unit = _place(n, me, size)
        load(0, n).wait()
        for event, when in ((None, 2), (LP, 3), (RP, 4)):
            @pl.when(n == when)
            def _():
                if event is not None:
                    arrived(0, event)
                load(0, n + 1).start()

        project(n, unit)

        def earlier(m, _):
            other = _place(m, me, size)
            pair(jnp.maximum(unit, other), jnp.minimum(unit, other), False)

        lax.fori_loop(0, n, earlier, None)
        pair(unit, unit, True)

        @pl.when(n == 0)
        def _():
            arrived(0, OWN)
            load(0, n + 1).start()

        @pl.when(n == 1)
        def _():
            passed_on(0)
            sides(0)
            for event in (L0, R1, L1, R0):
                sent(1, event).start()
            load(0, n + 1).start()

        @pl.when(n == 5)
        def _():
            far(0)
            load(0, n + 1).start()

        @pl.when(n == 6)
        def _():
            passed_on(1)
            arrived(0, OP)
            load(0, n + 1).start()

    lax.fori_loop(0, size, unit_step, None)
    saves = [pltpu.make_async_copy(a, b, save_sem.at[n]) for n, (a, b) in enumerate(((q_ref, q_out), (k_ref, k_out), (v_ref, v_out)))]
    for save in saves:
        save.start()
    keep(1).wait()
    load(1, 0).start()

    def save_do(n):
        here = pl.ds(pl.multiple_of(_place(n, me, size) * cols, cols), cols)
        return pltpu.make_async_copy(do_ref.at[:, here], do_out.at[:, here], do_sem.at[n])

    def finish(unit, _):
        for i in range(kb):
            for j in range(g):
                spot = pl.ds(pl.multiple_of(unit * cols + j * rows, rows), rows)
                total = mix_s[i, HEAD : HEAD + 1, spot]
                o = (mix_s[i, :HEAD, spot] * (1 / total)).T.astype(jnp.bfloat16)
                h = i * g + j
                o_s[at(unit), h * HEAD : (h + 1) * HEAD] = o
                lse_ref[i : i + 1, spot] = top_s[i : i + 1, spot] * HEAD**-0.5 + jnp.log(total)

    lax.fori_loop(0, size, finish, None)
    dwo_s[...] = jnp.zeros_like(dwo_s)

    def dy_step(n, _):
        unit = _place(n, me, size)
        load(1, n).wait()
        for event, when in ((None, 2), (LP, 3), (RP, 4)):
            @pl.when(n == when)
            def _():
                if event is not None:
                    arrived(1, event)
                load(1, n + 1).start()

        slot = lax.rem(n, 2)
        by_o = _dot(buf_s[slot], wo_ref[...], 1, 1).astype(jnp.bfloat16)
        o = o_s[at(unit), :]
        for i in range(kb):
            for j in range(g):
                h = i * g + j
                spot = pl.ds(pl.multiple_of(unit * cols + j * rows, rows), rows)
                mine = by_o[:, h * HEAD : (h + 1) * HEAD]
                do_ref[i, spot, :] = mine
                prod = mine.astype(jnp.float32) * o[:, h * HEAD : (h + 1) * HEAD].astype(jnp.float32)
                delta_ref[i : i + 1, spot] = prod.T.sum(axis=0, keepdims=True)

        save_do(n).start()

        def some(c, _):
            here = pl.ds(pl.multiple_of(c * 512, 512), 512)
            dwo_s[:, here] += _dot(o, buf_s[slot, :, here], 0, 0)

        lax.fori_loop(0, d // 512, some, None)

        @pl.when(n == 0)
        def _():
            arrived(1, OWN)
            load(1, n + 1).start()

        @pl.when(n == 1)
        def _():
            sides(1)
            load(1, n + 1).start()

        @pl.when(n == 5)
        def _():
            far(1)
            load(1, n + 1).start()

        @pl.when(n == 6)
        def _():
            arrived(1, OP)
            load(1, n + 1).start()

    lax.fori_loop(0, size, dy_step, None)
    dwo_ref[...] = dwo_s[...].astype(dwo_ref.dtype)
    for save in saves:
        save.wait()
    lax.fori_loop(0, size, lambda n, _: save_do(n).wait(), None)
    for a in range(2):
        for event in range(10):
            sent(a, event).wait_send()


def gather_forward(size, x, dy, gain, wq, wk, wv, wo):
    rows, d = x.shape
    total = rows * size
    kb, heads = wk.shape[1] // HEAD, wq.shape[1] // HEAD
    half = HEAD // 2
    rate = np.tile(np.float32(THETA) ** (-np.arange(half, dtype=np.float32) / half), 2)[None]
    bf16, f32 = jnp.bfloat16, jnp.float32
    vmem, hbm = pl.BlockSpec(memory_space=pltpu.VMEM), pl.BlockSpec(memory_space=pl.ANY)
    shape, dma = jax.ShapeDtypeStruct, pltpu.SemaphoreType.DMA
    width = heads // kb * total
    by_q, by_k, stats = (kb, width, HEAD), (kb, total, HEAD), (kb, width)
    return pl.pallas_call(
        functools.partial(_gather_forward, size),
        in_specs=[vmem] * 3 + [hbm] * 5,
        out_specs=[hbm] * 6 + [vmem] * 5,
        out_shape=[shape(s, bf16) for s in ((total, d), (total, d), by_q, by_k, by_k, by_q)]
        + [shape(stats, f32), shape(stats, f32), shape(wo.shape, bf16), shape((2, rows, HEAD), f32), shape((2, size, HEAD), f32)],
        scratch_shapes=[pltpu.VMEM(s, bf16) for s in (x.shape, wq.shape, wk.shape, wv.shape, wo.shape, by_q, by_k, by_k, by_q, x.shape,
                                                      (2, rows, d), (kb, HEAD + 16, total))]
        + [pltpu.VMEM(stats, f32), pltpu.VMEM((kb, HEAD + 16, width), f32), pltpu.VMEM((total, heads * HEAD), bf16), pltpu.VMEM(wo.shape, f32)]
        + [dma(s) for s in ((2, 10), (2, 10), (2,), (2,), (5,), (3,), (size,))],
        compiler_params=pltpu.CompilerParams(collective_id=0, has_side_effects=True, vmem_limit_bytes=62 * 2**20),
    )(x, gain.astype(f32)[None], jnp.asarray(rate), dy, wq, wk, wv, wo)


POINTS = (("", "", "70", "", "6071", "", "507261", "", "40736251", "", "30", "", "20635241", "", "1031", "", "00", "", "534221", "", "", "3211", "", "014322331202231303"),
          ("", "", "", "", "", "", "6050", "", "704051", "", "5230", "", "3153", "417161", "", "203210", "001172", "", "", "012133", "", "62", "", "22431342120273632303"))
ORDER = [[(int(a), int(b)) for point in points for a, b in zip(point[::2], point[1::2])] for points in POINTS]
STARTS = [[sum(len(point) for point in points[:n]) // 2 for n in range(len(points) + 1)] for points in POINTS]


def _pick(index, values):
    got = values[0]
    for n in range(1, len(values)):
        got = jnp.where(index == n, values[n], got)
    return got


def _backward(size, gain_ref, lse_ref, delta_ref, low_ref, high_ref, wq_in, wk_in, wv_in, q_ref, k_ref, v_ref, do_ref, xa_ref, x_ref, dy_ref,
              dx_ref, dgain_ref, dwq_ref, dwk_ref, dwv_ref,
              wq_ref, wk_ref, wv_ref, q_s, k_s, v_s, do_s, dq_s, dk_s, dv_s, tile_s, term_s, out_s, in_s, chain_s, last_s, stage_s, gain_s, gains_s,
              load_sem, do_sem, tile_sem, stage_sem, x_sem, out_sem, in_sem, chain_send, chain_recv, last_recv, gain_send, gain_recv):
    rows, d = x_ref.shape
    part = d // 2
    kb, g = k_ref.shape[0], q_ref.shape[1] // k_ref.shape[1]
    cols = g * rows
    pieces = [(i, j) for i in range(kb) for j in range(g)]
    chips = size // 2
    me = lax.axis_index("tp")
    core = lax.rem(me, 2)
    chip = lax.div(me, 2)
    partner = me + 1 - 2 * core
    onward = lax.rem(me + jnp.where(core == 0, 2, size - 2), size)
    scale = HEAD**-0.5
    e = scale * LOG2E
    bf16, f32 = jnp.bfloat16, jnp.float32
    subs = chain_recv.shape[1]
    sub = rows // subs

    barrier = pltpu.get_barrier_semaphore()
    for other in range(1, size):
        pl.semaphore_signal(barrier, inc=1, device_id={"tp": lax.rem(me + other, size)}, device_id_type=MESH)

    loads = [pltpu.make_async_copy(a, b, load_sem.at[n]) for n, (a, b) in enumerate(
        ((q_ref, q_s), (k_ref, k_s), (v_ref, v_s), (wq_in, wq_ref), (wk_in, wk_ref), (wv_in, wv_ref)))]
    for load in loads:
        load.start()

    def at(unit):
        return pl.ds(pl.multiple_of(unit * rows, rows), rows)

    def spot(unit, j):
        return pl.ds(pl.multiple_of(unit * cols + j * rows, rows), rows)

    def load_do(n):
        unit = size - 1 - n
        return pltpu.make_async_copy(do_ref.at[:, pl.ds(pl.multiple_of(unit * cols, cols), cols)], do_s.at[lax.rem(n, 2)], do_sem.at[lax.rem(n, 2)])

    def load_tile(n):
        width = tile_s.shape[2]
        return pltpu.make_async_copy(xa_ref.at[:, pl.ds(pl.multiple_of(n * width, width), width)], tile_s.at[lax.rem(n, 2)], tile_sem.at[lax.rem(n, 2)])

    load_do(0).start()

    def clear(j, _):
        for i in range(kb):
            dk_s[i, at(j), :] = jnp.zeros((rows, HEAD), f32)
            dv_s[i, at(j), :] = jnp.zeros((rows, HEAD), f32)

    lax.fori_loop(0, size, clear, None)
    pl.semaphore_wait(barrier, size - 1)
    for load in loads[:3]:
        load.wait()

    def pair(n, pq, pk, masked):
        slot = lax.rem(n, 2)
        keys = at(pk)
        if masked:
            ok = lax.broadcasted_iota(jnp.int32, (rows, rows), 1) >= lax.broadcasted_iota(jnp.int32, (rows, rows), 0)
        for i in range(kb):
            here = [slice(j * rows, (j + 1) * rows) for j in range(g)]
            qs = [q_s[i, spot(pq, j), :] for j in range(g)]
            dos = [do_s[slot, i, at_j, :] for at_j in here]
            scores = [_dot(k_s[i, keys, :], q, 1, 1) for q in qs]
            dps = [_dot(v_s[i, keys, :], do, 1, 1) for do in dos]
            for j in range(g):
                p = jnp.exp2(scores[j] * e - lse_ref[i : i + 1, spot(pq, j)] * LOG2E)
                if masked:
                    p = jnp.where(ok, p, 0.0)
                ds = (p * (dps[j] - delta_ref[i : i + 1, spot(pq, j)])).astype(bf16)
                dv_s[i, keys, :] += _dot(p.astype(bf16), dos[j], 1, 0)
                dk_s[i, keys, :] += _dot(ds, qs[j], 1, 0)
                new = _dot(k_s[i, keys, :].T, ds, 1, 0)
                dq_s[i, :, here[j]] = new if masked else dq_s[i, :, here[j]] + new

    def swap(unit):
        return pltpu.make_async_remote_copy(src_ref=out_s, dst_ref=in_s.at[unit], send_sem=out_sem, recv_sem=in_sem.at[unit],
                                            device_id={"tp": partner}, device_id_type=MESH)

    def pass_on(unit, s):
        here = pl.ds(s * sub, sub)
        return pltpu.make_async_remote_copy(src_ref=chain_s.at[unit, here], dst_ref=chain_s.at[unit, here], send_sem=chain_send.at[unit, s],
                                            recv_sem=chain_recv.at[unit, s], device_id={"tp": onward}, device_id_type=MESH)

    def hand_over(unit, s):
        here = pl.ds(s * sub, sub)
        return pltpu.make_async_remote_copy(src_ref=chain_s.at[unit, here], dst_ref=last_s.at[here], send_sem=chain_send.at[unit, s],
                                            recv_sem=last_recv.at[s], device_id={"tp": partner}, device_id_type=MESH)

    def turn_of(unit):
        away = jnp.where(core == 0, chip - lax.div(unit, 2), lax.div(unit, 2) - chip)
        return lax.rem(away + 2 * chips - 1, chips)

    def term(dq, dk, dv, first):
        here = pl.ds(pl.multiple_of(first, 256), 256)
        return _dot(dq, wq_ref[here, :], 1, 1) + _dot(dk, wk_ref[here, :], 1, 1) + _dot(dv, wv_ref[here, :], 1, 1)

    def by_heads(unit):
        dq = jnp.concatenate([q_s[i, spot(unit, j), :] for i, j in pieces], axis=1)
        return dq, *(jnp.concatenate([ref[i, at(unit), :] for i in range(kb)], axis=1) for ref in (k_s, v_s))

    def add_up(index, _):
        unit, turn = (jnp.where(core == 0, *(_pick(index, [entry[m] for entry in order]) for order in ORDER)) for m in range(2))

        @pl.when(turn_of(unit) == turn)
        def _():
            grads = by_heads(unit)
            for c in range(0, part, 256):
                term_s[:, c : c + 256] = term(*grads, core * part + c)
            swap(unit).wait_recv()
            for s in range(subs):
                here = pl.ds(s * sub, sub)
                mine = term_s[here, :] + in_s[unit, here, :].astype(f32)

                @pl.when(turn == 0)
                def _():
                    chain_s[unit, here, :] = mine.astype(bf16)

                @pl.when(turn > 0)
                def _():
                    pass_on(unit, s).wait_recv()
                    chain_s[unit, here, :] = (mine + chain_s[unit, here, :].astype(f32)).astype(bf16)

                @pl.when(turn < chips - 1)
                def _():
                    pass_on(unit, s).start()

                @pl.when((turn == chips - 1) & (lax.rem(unit, 2) != core))
                def _():
                    hand_over(unit, s).start()

    def point(n):
        first, end = (jnp.where(core == 0, *(_pick(at_n, starts) for starts in STARTS)) for at_n in (n, n + 1))
        lax.fori_loop(first, end, add_up, None)

    def step(n, _):
        unit = size - 1 - n
        load_do(n).wait()

        @pl.when(n < size - 1)
        def _():
            load_do(n + 1).start()

        pair(n, unit, unit, True)
        point(2 * n)
        lax.fori_loop(0, unit, lambda m, _: pair(n, unit, m, False), None)
        point(2 * n + 1)

        hc, hs = high_ref[0, pl.ds(unit, 1), :], high_ref[1, pl.ds(unit, 1), :]
        cos = low_ref[0] * hc - low_ref[1] * hs
        sin = low_ref[1] * hc + low_ref[0] * hs
        sin = sin * jnp.where(lax.broadcasted_iota(jnp.int32, (1, HEAD), 1) < HEAD // 2, 1.0, -1.0)

        def turn_back(t):
            t = (t * scale).astype(bf16).astype(f32)
            return (t * cos + pltpu.roll(t, HEAD // 2, 1) * sin).astype(bf16)

        for i, j in pieces:
            q_s[i, spot(unit, j), :] = turn_back(dq_s[i, :, j * rows : (j + 1) * rows].T)
        for i in range(kb):
            k_s[i, at(unit), :] = turn_back(dk_s[i, at(unit), :])
            v_s[i, at(unit), :] = dv_s[i, at(unit), :].astype(bf16)
        grads = by_heads(unit)

        @pl.when(n == 0)
        def _():
            for load in loads[3:]:
                load.wait()

        @pl.when(n > 0)
        def _():
            swap(unit).wait_send()

        for c in range(0, part, 256):
            out_s[:, c : c + 256] = term(*grads, (1 - core) * part + c).astype(bf16)
        swap(unit).start()

    lax.fori_loop(0, size, step, None)
    load_tile(0).start()
    swap(0).wait_send()
    width = tile_s.shape[2]
    tiles = d // width

    def late(m):
        return [pltpu.make_async_copy((x_ref, dy_ref)[m].at[:, pl.ds(n * width, width)], tile_s.at[m, pl.ds(n * rows, rows)], x_sem.at[m, n])
                for n in range(tiles)]


    def saves(n):
        slot, here, first = lax.rem(n, 2), pl.ds(pl.multiple_of(n * tile_s.shape[2], tile_s.shape[2]), tile_s.shape[2]), 0
        copies = []
        for m, ref in enumerate((dwq_ref, dwk_ref, dwv_ref)):
            copies.append(pltpu.make_async_copy(stage_s.at[slot, :, pl.ds(first, ref.shape[1])], ref.at[here, :], stage_sem.at[slot, m]))
            first += ref.shape[1]
        return copies

    def weights(n, _):
        width = tile_s.shape[2]
        load_tile(n).wait()

        @pl.when(n < tiles - 1)
        def _():
            load_tile(n + 1).start()

        here = pl.ds(pl.multiple_of(n * width, width), width)
        a = tile_s[lax.rem(n, 2)]
        slot = lax.rem(n, 2)

        @pl.when(n > 1)
        def _():
            for save in saves(n - 2):
                save.wait()

        for i in range(kb):
            total = 0
            for unit in range(size):
                b = jnp.concatenate([q_s[i, unit * cols + j * rows : unit * cols + (j + 1) * rows, :] for j in range(g)], axis=1)
                total += _dot(a[unit * rows : (unit + 1) * rows], b, 0, 0)
            stage_s[slot, :, i * g * HEAD : (i + 1) * g * HEAD] = total.astype(bf16)
        for m, ref in enumerate((k_s, v_s)):
            b = jnp.concatenate([ref[i] for i in range(kb)], axis=1)
            first = kb * g * HEAD + m * kb * HEAD
            stage_s[slot, :, first : first + kb * HEAD] = _dot(a, b, 0, 0).astype(bf16)
        for save in saves(n):
            save.start()
        for m in range(2):
            @pl.when(n == tiles - 2 + m)
            def _():
                for load in late(m):
                    load.start()

        point(2 * size + n)

    lax.fori_loop(0, tiles, weights, None)

    for s in range(subs):
        hand_over(me, s).wait_recv()

    gain_s[...] = jnp.zeros_like(gain_s)
    for load in late(0) + late(1):
        load.wait()

    def norm(j, _):
        here = pl.ds(pl.multiple_of(j * 64, 64), 64)
        mine, other = chain_s[me, here, :], last_s[here, :]
        by = jnp.concatenate([jnp.where(core == 0, mine, other), jnp.where(core == 0, other, mine)], axis=1).astype(f32)
        wide, given = (jnp.concatenate([tile_s[m, pl.ds(n * rows + j * 64, 64)] for n in range(tiles)], axis=1).astype(f32) for m in range(2))
        size_of = lax.rsqrt(jnp.mean(wide * wide, -1, keepdims=True) + 1e-6)
        normal = wide * size_of
        gain_s[...] += (by * normal).reshape(8, 8, d).sum(axis=0)
        by = by * gain_ref[...]
        by = size_of * (by - normal * jnp.mean(by * normal, -1, keepdims=True))
        by = (by + given).astype(bf16)
        in_s[0, here, :], in_s[1, here, :] = by[:, :part], by[:, part:]

    lax.fori_loop(0, rows // 64, norm, None)

    def tell(other):
        return pltpu.make_async_remote_copy(src_ref=gain_s, dst_ref=gains_s.at[me], send_sem=gain_send.at[other], recv_sem=gain_recv.at[other],
                                            device_id={"tp": lax.rem(me + other, size)}, device_id_type=MESH)

    def heard(other):
        source = lax.rem(me + size - other, size)
        return pltpu.make_async_remote_copy(src_ref=gain_s, dst_ref=gains_s.at[source], send_sem=gain_send.at[other], recv_sem=gain_recv.at[other],
                                            device_id={"tp": lax.rem(me + other, size)}, device_id_type=MESH)

    for other in range(1, size):
        tell(other).start()
    results = [pltpu.make_async_copy(in_s.at[n], dx_ref.at[:, pl.ds(n * part, part)], x_sem.at[0, n]) for n in range(2)]
    for save in results:
        save.start()
    gains_s[me] = gain_s[...]
    for other in range(1, size):
        heard(other).wait_recv()
    total = gains_s[0]
    for other in range(1, size):
        total += gains_s[other]
    dgain_ref[...] = total.sum(axis=0, keepdims=True)
    for other in range(1, size):
        tell(other).wait_send()
    for save in (*results, *saves(tiles - 2), *saves(tiles - 1)):
        save.wait()

    def sent(unit, _):
        final = turn_of(unit) == chips - 1

        @pl.when(jnp.logical_not(final))
        def _():
            for s in range(subs):
                pass_on(unit, s).wait_send()

        @pl.when(final & (lax.rem(unit, 2) != core))
        def _():
            for s in range(subs):
                hand_over(unit, s).wait_send()

    lax.fori_loop(0, size, sent, None)


def backward(size, x, dy, gain, lse, delta, wq, wk, wv, tables, q, k, v, do, xa):
    rows, d = x.shape
    kb, total = k.shape[:2]
    cols = q.shape[1] // size
    bf16, f32 = jnp.bfloat16, jnp.float32
    vmem, hbm = pl.BlockSpec(memory_space=pltpu.VMEM), pl.BlockSpec(memory_space=pl.ANY)
    shape, dma, subs, width = jax.ShapeDtypeStruct, pltpu.SemaphoreType.DMA, 4, 256
    return pl.pallas_call(
        functools.partial(_backward, size),
        in_specs=[vmem] * 5 + [hbm] * 10,
        out_specs=[hbm, vmem, hbm, hbm, hbm],
        out_shape=[shape((rows, d), bf16), shape((1, d), f32)] + [shape(w.shape, bf16) for w in (wq, wk, wv)],
        scratch_shapes=[pltpu.VMEM(w.shape, bf16) for w in (wq, wk, wv)] + [
                        pltpu.VMEM(q.shape, bf16), pltpu.VMEM(k.shape, bf16), pltpu.VMEM(v.shape, bf16), pltpu.VMEM((2, kb, cols, HEAD), bf16),
                        pltpu.VMEM((kb, HEAD, cols), f32), pltpu.VMEM(k.shape, f32), pltpu.VMEM(v.shape, f32), pltpu.VMEM((2, total, width), bf16),
                        pltpu.VMEM((rows, d // 2), f32), pltpu.VMEM((rows, d // 2), bf16), pltpu.VMEM((size, rows, d // 2), bf16),
                        pltpu.VMEM((size, rows, d // 2), bf16), pltpu.VMEM((rows, d // 2), bf16), pltpu.VMEM((2, width, sum(w.shape[1] for w in (wq, wk, wv))), bf16), pltpu.VMEM((8, d), f32),
                        pltpu.VMEM((size, 8, d), f32),
                        dma((6,)), dma((2,)), dma((2,)), dma((2, 3)), dma((2, d // width)), dma, dma((size,)), dma((size, subs)), dma((size, subs)), dma((subs,)), dma((size,)), dma((size,))],
        compiler_params=pltpu.CompilerParams(collective_id=1, has_side_effects=True, vmem_limit_bytes=67043328),
    )(gain.astype(f32)[None], lse, delta, *tables, wq, wk, wv, q, k, v, do, xa, x, dy)


def solution(mesh):
    size = mesh.shape["tp"]

    def step(x, dy, gain, wq, wk, wv, wo):
        xa, _, q, k, v, do, lse, delta, dwo, *tables = gather_forward(size, x, dy, gain, wq, wk, wv, wo)
        dx, dgain, dwq, dwk, dwv = backward(size, x, dy, gain, lse, delta, wq, wk, wv, tables, q, k, v, do, xa)
        return dx, dgain, dwq, dwk, dwv, dwo

    tokens, columns = P(("dp", "tp"), None), P(None, "tp")
    return jax.shard_map(
        step,
        mesh=mesh,
        in_specs=(tokens, tokens, P(None), columns, columns, columns, P("tp", None)),
        out_specs=(tokens, P("dp", None), P("dp", "tp"), P("dp", "tp"), P("dp", "tp"), P(("dp", "tp"), None)),
        check_vma=False,
    )
```
